32 devices in a mesh: dp: 4 (over x, core), tensor: 8 (over z, y).
Axes of the slice: x: 2, y: 2, z: 4, core: 2. Of those that a mesh axis runs over, the one named last changes fastest.
Arguments:
- activations: bfloat16 [1024, 5120], P('dp'), may hold values from -6 to 6
- grad_out: bfloat16 [1024, 5120], P('dp'), may hold values from -6 to 6
- gate_pre: bfloat16 [1024, 7168], P('dp', 'tensor'), may hold values from -8 to 8
- up_pre: bfloat16 [1024, 7168], P('dp', 'tensor'), may hold values from -6 to 6
- gate_up: bfloat16 [5120, 2, 7168], P('dp', None, 'tensor'), may hold values from -0.078125 to 0.078125
- down_weight: bfloat16 [5120, 7168], P('dp', 'tensor'), may hold values from -0.0625 to 0.0625
Outputs:
- grad_input: bfloat16 [1024, 5120], P('dp')
- grad_gate_up: float32 [5120, 2, 7168], P('dp', None, 'tensor')
- grad_down: float32 [5120, 7168], P('dp', 'tensor')
The draws below stay inside these ranges and needn't reach their ends.
All inputs are finite; a program needn't handle non-finite values.
Results may differ from the reference program's by a relative error of at most 0.017.
Values may be sent and summed in bfloat16 or wider, within the bound.
A program may use at most 128 MiB of HBM per device.

```python
import jax
import jax.numpy as jnp
from jax import lax

D = 5120
FF = 7168
TOK_DEV = 256
TOKENS = 1024
N_DP = 4
N_TENSOR = 8


def raised(result, stream_key, source, target, blocks, factor):
    owner, partner = [(jnp.arange(result.shape[dim]) // (result.shape[dim] // blocks)).reshape([-1 if axis == dim else 1 for axis in range(result.ndim)]) for dim in (source, target)]
    chosen = jax.random.permutation(stream_key, blocks)[partner]
    strong = (owner == chosen) | (owner == (partner + blocks // 2) % blocks)
    return jnp.where(strong, factor * result, result)


def shard_levels(own_key, extent, cuts, low, high):
    def one(dim, shards_of):
        draws = jax.random.uniform(jax.random.fold_in(jax.random.fold_in(own_key, 6), dim), (shards_of,), jnp.float32, low / len(cuts), high / len(cuts))
        return jnp.repeat(jnp.exp(draws), extent[dim] // shards_of).reshape((-1,) + (1,) * (len(extent) - dim - 1))

    gain = one(*cuts[0])
    for cut in cuts[1:]:
        gain = gain * one(*cut)
    return gain


def scatter_about(own_key, dims, scale, bound, shards=(), kind=jnp.bfloat16):
    array = jax.random.normal(own_key, dims, jnp.float32) * scale
    if len(shards) > 0:
        array = shard_levels(own_key, dims, shards, -0.22, 0.18) * array
    return jnp.clip(array, min=-bound, max=bound).astype(kind)


def gaussian_with(key, shape, scale, bound, split, heavy, kind=jnp.bfloat16):
    drawn = scale * jax.random.normal(key, shape, jnp.float32)
    if split:
        drawn = drawn * shard_levels(key, shape, split, -0.22, 0.18)
    return jnp.clip(raised(drawn, jax.random.fold_in(key, 3), *heavy), -bound, bound).astype(kind)


def setup_inputs(seed: int = 0) -> dict:
    key_list = jax.random.split(jax.random.key(seed), 7)
    return {
        "activations": gaussian_with(key_list[0], (TOKENS, D), 1.0, 6.0, ((0, 4),), (0, 1, 4, 2.0)),
        "grad_out": gaussian_with(key_list[1], (TOKENS, D), 1.0, 6.0, ((0, 4),), (0, 1, 4, 2.0)),
        "gate_pre": scatter_about(key_list[2], (TOKENS, FF), 1.5, 8.0, ((0, 4), (1, 8))),
        "up_pre": scatter_about(key_list[3], (TOKENS, FF), 1.0, 6.0, ((0, 4), (1, 8))),
        "gate_up": scatter_about(key_list[4], (D, 2, FF), D ** -0.5, 0.078125, ((0, 4), (2, 8))),
        "down_weight": scatter_about(key_list[5], (D, FF), FF ** -0.5, 0.0625, ((0, 4), (1, 8))),
    }


def reference(activations, grad_out, gate_pre, up_pre, gate_up, down_weight):
    gate_wide = gate_pre.astype(jnp.float32)
    up_wide = up_pre.astype(jnp.float32)
    gate_sigmoid = jax.nn.sigmoid(gate_wide)
    gate_silu = gate_wide * gate_sigmoid
    hidden = (gate_silu * up_wide).astype(jnp.bfloat16)
    grad_h = jnp.dot(grad_out, down_weight, preferred_element_type=jnp.float32)
    grad_gate = grad_h * up_wide * gate_sigmoid * (1.0 + gate_wide * (1.0 - gate_sigmoid))
    grad_up = grad_h * gate_silu
    grad_hidden = jnp.stack([grad_gate, grad_up], axis=1).astype(jnp.bfloat16)

    group_width = FF // N_TENSOR
    hidden_groups = grad_hidden.reshape(TOKENS, 2, N_TENSOR, group_width).transpose(2, 0, 1, 3)
    hidden_groups = hidden_groups.reshape(N_TENSOR, TOKENS, 2 * group_width)
    weight_groups = gate_up.reshape(D, 2, N_TENSOR, group_width).transpose(2, 0, 1, 3)
    weight_groups = weight_groups.reshape(N_TENSOR, D, 2 * group_width)

    def add_part(running, paired):
        left_rows, right_rows = paired
        part_sum = jnp.dot(left_rows, right_rows.T, preferred_element_type=jnp.float32)
        part_sum = lax.optimization_barrier(part_sum.astype(jnp.bfloat16))
        return running + part_sum.astype(jnp.float32), None

    input_total, _ = lax.scan(add_part, jnp.zeros((TOKENS, D), jnp.float32), (hidden_groups, weight_groups))
    grad_input = input_total.astype(jnp.bfloat16)

    act_groups = activations.reshape(N_DP, TOK_DEV, D)
    out_groups = grad_out.reshape(N_DP, TOK_DEV, D)
    grad_groups = grad_hidden.reshape(N_DP, TOK_DEV, 2 * FF)
    plain_groups = hidden.reshape(N_DP, TOK_DEV, FF)

    def add_group(running, group_items):
        act_rows, out_rows, grad_rows, plain_rows = group_items
        gate_part = jnp.dot(act_rows.T, grad_rows, preferred_element_type=jnp.float32)
        down_part = jnp.dot(out_rows.T, plain_rows, preferred_element_type=jnp.float32)
        gate_part = lax.optimization_barrier(gate_part.astype(jnp.bfloat16))
        down_part = lax.optimization_barrier(down_part.astype(jnp.bfloat16))
        return (running[0] + gate_part.astype(jnp.float32), running[1] + down_part.astype(jnp.float32)), None

    start_sums = (jnp.zeros((D, 2 * FF), jnp.float32), jnp.zeros((D, FF), jnp.float32))
    summed, _ = lax.scan(add_group, start_sums, (act_groups, out_groups, grad_groups, plain_groups))
    grad_gate_up = (summed[0] / N_DP).reshape(D, 2, FF)
    grad_down = summed[1] / N_DP
    return grad_input, grad_gate_up, grad_down
```

```python
import jax
import jax.numpy as jnp
from jax import lax
from jax.experimental import pallas as pl
from jax.experimental.pallas import tpu as pltpu
from jax.sharding import PartitionSpec as P

MESH = pl.DeviceIdType.MESH
ANY = pl.BlockSpec(memory_space=pl.ANY)
VMEM = pl.BlockSpec(memory_space=pltpu.VMEM)
F32 = jnp.float32
BF16 = jnp.bfloat16


def remote(src, dst, send, recv, device):
    return pltpu.make_async_remote_copy(
        src_ref=src, dst_ref=dst, send_sem=send, recv_sem=recv, device_id=device, device_id_type=MESH
    )


def tile_of(size):
    for tile in (256, 128):
        if size % tile == 0:
            return tile
    return size


class Line:
    def __init__(self, block, send, recv, j, m):
        self.block, self.send, self.recv = block, send, recv
        self.m, self.lines = m, m // 2
        self.row, self.column = j // 2, lax.rem(j, 2)
        self.facing = j + 1 - 2 * self.column
        self.above_me, self.below_me = lax.rem(j + 2, m), lax.rem(j + m - 2, m)
        self.first, self.last = self.row == 0, self.row == self.lines - 1

    def hop(self, kind, r, device):
        k = 2 * r + self.column
        block = self.block(k)
        return remote(block, block, self.send.at[kind, r], self.recv.at[k], {"tensor": device})

    def up(self, r):
        return self.hop(0, r, self.above_me)

    def down(self, r):
        return self.hop(1, r, self.below_me)

    def across(self, r):
        return self.hop(2, r, self.facing)

    def step(self, d):
        below, above = self.row - d, self.row + d

        @pl.when(below >= 0)
        def _():
            if d > 0:
                self.up(below).wait_recv()
            pl.when(jnp.logical_not(self.last))(lambda: self.up(below).start())
            if d == 0:
                pl.when(jnp.logical_not(self.first))(lambda: self.down(self.row).start())
            self.across(below).start()

        if d > 0:

            @pl.when(above < self.lines)
            def _():
                self.down(above).wait_recv()
                pl.when(jnp.logical_not(self.first))(lambda: self.down(above).start())
                self.across(above).start()

    def finish(self):
        for r in range(self.lines):
            k = 2 * r + 1 - self.column
            block = self.block(k)
            remote(
                block, block, self.send.at[2, r], self.recv.at[k], {"tensor": self.facing}
            ).wait_recv()

    def drain(self):
        for r in range(self.lines):
            self.across(r).wait_send()
            went_up = jnp.logical_and(jnp.logical_not(self.last), r <= self.row)
            went_down = jnp.logical_and(jnp.logical_not(self.first), r >= self.row)
            pl.when(went_up)(lambda: self.up(r).wait_send())
            pl.when(went_down)(lambda: self.down(r).wait_send())


def layer(cid, activations, grad_out, gate_pre, up_pre, gate_w, up_w, down_w):
    tokens, model = activations.shape
    slab, width = down_w.shape
    n = lax.axis_size("dp")
    m = lax.axis_size("tensor")
    chips, lines = n // 2, m // 2
    rows = tokens // m
    aligned = slab % 128 == 0
    if not aligned:
        activations, grad_out = (
            a.reshape(tokens, n, slab).transpose(1, 0, 2) for a in (activations, grad_out)
        )
    tile = tile_of(slab)
    tiles = slab // tile
    lot = 16

    def kernel(
        x_in, dy_in, gate_in, up_in, w0_in, w1_in, down_in,
        out, wg0, wg1, wd,
        dy, x, gate, up, grad_h, down, w0, w1,
        keep, swap, pair, came, part, beside, carry, rising, falling, mine, final,
        wbuf,
        line_s, line_r, hop_s, hop_r, ge_s, ge_r, pair_s, pair_r, ex_s, ex_r, g_s, g_r,
        y_s, y_r, z_s, up_r, dn_r, load, store,
    ):
        me = lax.axis_index("dp")
        j = lax.axis_index("tensor")
        core = lax.rem(me, 2)
        chip = me // 2
        partner = me + 1 - 2 * core
        z, y = j // 2, lax.rem(j, 2)
        facing = j + 1 - 2 * y
        above, below = lax.rem(j + 2, m), lax.rem(j + m - 2, m)
        first, last = z == 0, z == lines - 1

        def shifted(s):
            return lax.rem(chip + s, chips)

        barrier = pltpu.get_barrier_semaphore()

        def signal(device):
            pl.semaphore_signal(barrier, inc=1, device_id=device, device_id_type=MESH)

        for s in range(1, n):
            signal({"dp": lax.rem(me + s, n)})
        signal({"tensor": facing})
        pl.when(jnp.logical_not(first))(lambda: signal({"tensor": below}))
        pl.when(jnp.logical_not(last))(lambda: signal({"tensor": above}))
        pl.semaphore_wait(barrier, n + (z > 0).astype(jnp.int32) + (z < lines - 1).astype(jnp.int32))

        def own_rows(ref, p):
            r = pl.ds(pl.multiple_of(j * rows, rows), rows)
            if aligned:
                return ref.at[r, pl.ds(pl.multiple_of(p * slab, 128), slab)]
            return ref.at[p, r]

        def own_all(ref, p):
            if aligned:
                return ref.at[:, pl.ds(pl.multiple_of(p * slab, 128), slab)]
            return ref.at[p]

        def block(buf, p, k):
            return buf.at[p, pl.ds(pl.multiple_of(k * rows, rows), rows)]

        def pair_block(buf, c, k):
            return buf.at[pl.ds(2 * c, 2), pl.ds(pl.multiple_of(k * rows, rows), rows)]

        local_loads = [
            pltpu.make_async_copy(src, dst, load.at[i])
            for i, (src, dst) in enumerate(
                ((down_in, down), (w0_in, w0), (w1_in, w1), (gate_in, gate.at[me]), (up_in, up.at[me]))
            )
        ]

        def hop_copy(b, src, buf, p):
            return remote(own_rows(src, p), block(buf, me, j), hop_s.at[b, p], hop_r.at[b, me], {"dp": p})

        def hop_whole(b, src, buf):
            return remote(
                own_all(src, partner), buf.at[me], hop_s.at[b, partner], hop_r.at[b, me], {"dp": partner}
            )

        def hop_own(b, src, buf):
            return pltpu.make_async_copy(own_all(src, me), buf.at[me], hop_s.at[b, me])

        def hop_start(b, src, buf):
            for s in range(1, chips):
                for c in range(2):
                    hop_copy(b, src, buf, 2 * shifted(s) + c).start()
            hop_whole(b, src, buf).start()
            hop_own(b, src, buf).start()

        def hop_arrive(b, buf):
            for s in range(1, chips):
                for c in range(2):
                    q = 2 * shifted(s) + c
                    spot = block(buf, q, j)
                    remote(spot, spot, hop_s.at[b, q], hop_r.at[b, q], {"dp": q}).wait_recv()

        def hop_near(b, src, buf):
            hop_own(b, src, buf).wait()
            spot = buf.at[partner]
            remote(spot, spot, hop_s.at[b, partner], hop_r.at[b, partner], {"dp": partner}).wait_recv()

        def hop_drain(b, src, buf):
            for s in range(1, chips):
                for c in range(2):
                    hop_copy(b, src, buf, 2 * shifted(s) + c).wait_send()
            hop_whole(b, src, buf).wait_send()

        def wide_copy(a, src, buf, s):
            q = partner if s == 0 else 2 * shifted(s) + core
            return remote(src, buf.at[me], ge_s.at[a, s], ge_r.at[a, me], {"dp": q})

        def wide_forward(a, buf, s):
            q = 2 * shifted(s) + core
            return remote(buf.at[q], buf.at[q], ge_s.at[a, chips + s], ge_r.at[a, q], {"dp": partner})

        def wide_wait(a, buf, q):
            remote(buf.at[q], buf.at[q], ge_s.at[a, 0], ge_r.at[a, q], {"dp": q}).wait_recv()

        local_loads[0].start()
        hop_start(0, dy_in, dy)
        for s in range(1, chips):
            wide_copy(0, gate_in, gate, s).start()
        hop_start(1, x_in, x)
        for s in range(1, chips):
            wide_copy(1, up_in, up, s).start()
        wide_copy(0, gate_in, gate, 0).start()
        wide_copy(1, up_in, up, 0).start()
        for copy in local_loads[1:]:
            copy.start()

        def lines_of(buf, base, shifts):
            made = []
            for i, s in enumerate(shifts):
                c = shifted(s)
                made.append(
                    Line(
                        lambda k, c=c: pair_block(buf, c, k),
                        line_s.at[base + i],
                        line_r.at[base + i],
                        j,
                        m,
                    )
                )
            return made

        others = list(range(1, chips))
        dy_lines = lines_of(dy, 0, others)
        x_lines = lines_of(x, chips - 1, others)
        out_lines = lines_of(out, 2 * chips - 2, others + [0])

        def all_of(made, name, *args):
            for line in made:
                getattr(line, name)(*args)

        def multiply(c):
            got = 2 * c + 1 - core
            swap[c] = jnp.dot(dy[got], down[...], preferred_element_type=F32).astype(BF16)
            pair_copy(c).start()
            keep[c] = jnp.dot(dy[2 * c + core], down[...], preferred_element_type=F32)

        def pair_copy(c):
            return remote(swap.at[c], pair.at[c], pair_s.at[c], pair_r.at[c], {"dp": partner})

        def ex_copy(c, s):
            q = 2 * shifted(s) + core
            return remote(swap.at[c], came.at[chip, c], ex_s.at[c, s], ex_r.at[c, chip], {"dp": q})

        def chip_sum(c):
            pair_copy(c).wait()

            @pl.loop(0, tokens // lot)
            def _(i):
                r = pl.ds(i * lot, lot)
                total = keep[c, r] + pair[c, r].astype(F32)
                keep[c, r] = total
                swap[c, r] = total.astype(BF16)

            for s in others:
                ex_copy(c, s).start()

        def g_copy(c):
            spot = grad_h.at[2 * c + core]
            return remote(spot, spot, g_s.at[c], g_r.at[c], {"dp": partner})

        def grad_h_sum(c):
            for s in others:
                q = shifted(s)
                spot = came.at[q, c]
                remote(spot, spot, ex_s.at[c, s], ex_r.at[c, q], {"dp": 2 * q + core}).wait_recv()

            @pl.loop(0, tokens // lot)
            def _(i):
                r = pl.ds(i * lot, lot)
                total = keep[c, r]
                for s in others:
                    total = total + came[shifted(s), c, r].astype(F32)
                grad_h[2 * c + core, r] = total.astype(BF16)

            g_copy(c).start()

        def gates(p):
            @pl.loop(0, tokens // lot)
            def _(i):
                r = pl.ds(i * lot, lot)
                v = gate[p, r].astype(F32)
                u = up[p, r].astype(F32)
                g = grad_h[p, r].astype(F32)
                s = jax.nn.sigmoid(v)
                silu = v * s
                grad_h[p, r] = (silu * u).astype(BF16)
                gate[p, r] = (g * u * s * (1.0 + v * (1.0 - s))).astype(BF16)
                up[p, r] = (g * silu).astype(BF16)

        def input_part(c):
            across = (((1,), (1,)), ((), ()))
            left0 = gate[pl.ds(2 * c, 2)].reshape(2 * tokens, width)
            left1 = up[pl.ds(2 * c, 2)].reshape(2 * tokens, width)
            for i in range(tiles):
                cols = pl.ds(i * tile, tile)
                total = lax.dot_general(left0, w0[cols], across, preferred_element_type=F32)
                total = total + lax.dot_general(left1, w1[cols], across, preferred_element_type=F32)
                part[c, :, :, cols] = total.astype(BF16).reshape(2, tokens, tile)

        def target(i):
            return jnp.where(z < lines // 2, lines - 1 - i, i)

        def y_copy(c, i):
            t = target(i)
            k = 2 * t + 1 - y
            src = part.at[c, :, pl.ds(pl.multiple_of(k * rows, rows), rows)]
            return remote(src, beside.at[c, t], y_s.at[c, t], y_r.at[c, t], {"tensor": facing})

        def climb(c, t):
            return remote(carry.at[c, t], rising.at[c, t], z_s.at[c, t], up_r.at[c, t], {"tensor": above})

        def descend(c, t):
            return remote(carry.at[c, t], falling.at[c, t], z_s.at[c, t], dn_r.at[c, t], {"tensor": below})

        def add_rows(fn):
            for g in range(2):
                for i in range(rows // lot):
                    fn(g, slice(i * lot, (i + 1) * lot), i * lot)

        def item(c, i):
            t = target(i)
            y_copy(c, i).wait_recv()
            rise = jnp.logical_and(t > z, z > 0)
            fall = jnp.logical_and(t < z, z < lines - 1)
            pl.when(rise)(lambda: climb(c, t).wait_recv())
            pl.when(fall)(lambda: descend(c, t).wait_recv())

            def start_of(g, r0):
                r = pl.ds(pl.multiple_of((2 * t + y) * rows + r0, lot), lot)
                return part[c, g, r].astype(F32)

            def plain(g, r, r0):
                carry[c, t, g, r] = (start_of(g, r0) + beside[c, t, g, r].astype(F32)).astype(BF16)

            def risen(g, r, r0):
                total = start_of(g, r0) + beside[c, t, g, r].astype(F32)
                carry[c, t, g, r] = (total + rising[c, t, g, r].astype(F32)).astype(BF16)

            def fallen(g, r, r0):
                total = start_of(g, r0) + beside[c, t, g, r].astype(F32)
                carry[c, t, g, r] = (total + falling[c, t, g, r].astype(F32)).astype(BF16)

            def own(g, r, r0):
                mine[c, g, r] = start_of(g, r0) + beside[c, t, g, r].astype(F32)

            pl.when(rise)(lambda: add_rows(risen))
            pl.when(fall)(lambda: add_rows(fallen))
            edge = jnp.logical_or(
                jnp.logical_and(first, t > z), jnp.logical_and(last, t < z)
            )
            pl.when(edge)(lambda: add_rows(plain))
            pl.when(t == z)(lambda: add_rows(own))
            pl.when(t > z)(lambda: climb(c, t).start())
            pl.when(t < z)(lambda: descend(c, t).start())

        def total_of(c):
            pl.when(z > 0)(lambda: climb(c, z).wait_recv())
            pl.when(z < lines - 1)(lambda: descend(c, z).wait_recv())

            def close(parts):
                def fn(g, r, r0):
                    total = mine[c, g, r]
                    for ref in parts:
                        total = total + ref[c, z, g, r].astype(F32)
                    final[c, g, r] = total.astype(BF16)

                return fn

            pl.when(first)(lambda: add_rows(close((falling,))))
            pl.when(last)(lambda: add_rows(close((rising,))))
            inner = jnp.logical_not(jnp.logical_or(first, last))
            pl.when(inner)(lambda: add_rows(close((rising, falling))))

        def out_copy(c, g):
            p = 2 * c + g
            return remote(final.at[c, g], block(out, me, j), hop_s.at[2, p], hop_r.at[2, me], {"dp": p})

        def out_send(s):
            c = shifted(s)
            if s > 0:
                for g in range(2):
                    out_copy(c, g).start()
            else:
                out_copy(c, 1 - core).start()
                pltpu.make_async_copy(final.at[c, core], block(out, me, j), hop_s.at[2, me]).start()

        def out_arrive(s):
            c = shifted(s)
            if s > 0:
                for g in range(2):
                    q = 2 * c + g
                    spot = block(out, q, j)
                    remote(spot, spot, hop_s.at[2, q], hop_r.at[2, q], {"dp": q}).wait_recv()
            else:
                spot = block(out, partner, j)
                remote(
                    spot, spot, hop_s.at[2, partner], hop_r.at[2, partner], {"dp": partner}
                ).wait_recv()
                pltpu.make_async_copy(final.at[c, core], block(out, me, j), hop_s.at[2, me]).wait()

        def out_drain(s):
            c = shifted(s)
            for g in range(2):
                if s > 0:
                    out_copy(c, g).wait_send()
            if s == 0:
                out_copy(c, 1 - core).wait_send()

        def stored(i):
            rows_i = pl.ds(i * tile, tile)
            return [
                pltpu.make_async_copy(wbuf.at[a, rows_i], ref.at[rows_i], store.at[a, i])
                for a, ref in enumerate((wg0, wg1, wd))
            ]

        def weights(i):
            down_cols = (((0,), (0,)), ((), ()))
            cols = pl.ds(i * tile, tile)
            left = x[:, :, cols].reshape(n * tokens, tile)
            back = dy[:, :, cols].reshape(n * tokens, tile)
            for a, (lhs, ref) in enumerate(((left, gate), (left, up), (back, grad_h))):
                total = lax.dot_general(
                    lhs, ref[...].reshape(n * tokens, width), down_cols, preferred_element_type=F32
                )
                wbuf[a, cols] = (total * (1.0 / n)).astype(BF16)
            for copy in stored(i):
                copy.start()

        hop_arrive(0, dy)
        all_of(dy_lines, "step", 0)
        hop_near(0, dy_in, dy)
        local_loads[0].wait()
        multiply(chip)
        if lines > 1:
            all_of(dy_lines, "step", 1)
        chip_sum(chip)
        for d in range(2, lines):
            all_of(dy_lines, "step", d)
        hop_arrive(1, x)
        all_of(x_lines, "step", 0)
        all_of(dy_lines, "finish")
        for s in others:
            multiply(shifted(s))
        for s in others:
            chip_sum(shifted(s))
        for d in range(1, lines):
            all_of(x_lines, "step", d)
        for s in others:
            q = 2 * shifted(s) + core
            wide_wait(0, gate, q)
            wide_forward(0, gate, s).start()
        for s in others:
            q = 2 * shifted(s) + core
            wide_wait(1, up, q)
            wide_forward(1, up, s).start()
        local_loads[1].wait()
        local_loads[2].wait()
        for s in others + [0]:
            c = shifted(s)
            grad_h_sum(c)
            if s == 0:
                local_loads[3].wait()
                local_loads[4].wait()
            else:
                wide_forward(0, gate, s).wait_send()
                wide_forward(1, up, s).wait_send()
            wide_wait(0, gate, 2 * c + 1 - core)
            wide_wait(1, up, 2 * c + 1 - core)
            g_copy(c).wait_send()
            gates(2 * c + core)
            spot = grad_h.at[2 * c + 1 - core]
            remote(spot, spot, g_s.at[c], g_r.at[c], {"dp": partner}).wait_recv()
            gates(2 * c + 1 - core)
            input_part(c)
            for i in range(lines):
                y_copy(c, i).start()
        all_of(x_lines, "finish")
        hop_near(1, x_in, x)

        spare = list(range(tiles))

        def some(count):
            for _ in range(count):
                if spare:
                    weights(spare.pop(0))

        for s in others:
            for i in range(lines):
                item(shifted(s), i)
            total_of(shifted(s))
            out_send(s)
        some(1)
        half = lines // 2
        for i in range(half):
            item(chip, i)
        for s in others:
            out_arrive(s)
        all_of(out_lines[:-1], "step", 0)
        for i in range(half, lines):
            item(chip, i)
        some(1)
        total_of(chip)
        out_send(0)
        if lines > 1:
            all_of(out_lines[:-1], "step", 1)
        out_arrive(0)
        out_lines[-1].step(0)
        some(1)
        for d in range(2, lines + 1):
            if d < lines:
                all_of(out_lines[:-1], "step", d)
            if d - 1 < lines and d > 1:
                out_lines[-1].step(d - 1)
            some(1)
        some(tiles)
        all_of(out_lines, "finish")

        all_of(dy_lines + x_lines + out_lines, "drain")
        hop_drain(0, dy_in, dy)
        hop_drain(1, x_in, x)
        for s in range(chips):
            wide_copy(0, gate_in, gate, s).wait_send()
            wide_copy(1, up_in, up, s).wait_send()
            for u in others:
                ex_copy(shifted(s), u).wait_send()
            for i in range(lines):
                y_copy(shifted(s), i).wait_send()
                t = target(i)
                pl.when(t > z)(lambda: climb(shifted(s), t).wait_send())
                pl.when(t < z)(lambda: descend(shifted(s), t).wait_send())
            out_drain(s)
        for i in range(tiles):
            for copy in stored(i):
                copy.wait()

    dma = pltpu.SemaphoreType.DMA
    vm = pltpu.VMEM
    flops = 2 * n * tokens * slab * width * 6
    return pl.pallas_call(
        kernel,
        out_shape=[jax.ShapeDtypeStruct((n, tokens, slab), BF16)]
        + [jax.ShapeDtypeStruct((slab, width), BF16)] * 3,
        in_specs=[ANY] * 7,
        out_specs=[VMEM] + [ANY] * 3,
        scratch_shapes=[
            vm((n, tokens, slab), BF16),
            vm((n, tokens, slab), BF16),
            vm((n, tokens, width), BF16),
            vm((n, tokens, width), BF16),
            vm((n, tokens, width), BF16),
            vm((slab, width), BF16),
            vm((slab, width), BF16),
            vm((slab, width), BF16),
            vm((chips, tokens, width), F32),
            vm((chips, tokens, width), BF16),
            vm((chips, tokens, width), BF16),
            vm((chips, chips, tokens, width), BF16),
            vm((chips, 2, tokens, slab), BF16),
            vm((chips, lines, 2, rows, slab), BF16),
            vm((chips, lines, 2, rows, slab), BF16),
            vm((chips, lines, 2, rows, slab), BF16),
            vm((chips, lines, 2, rows, slab), BF16),
            vm((chips, 2, rows, slab), F32),
            vm((chips, 2, rows, slab), BF16),
            vm((3, slab, width), BF16),
            dma((3 * chips - 2, 3, lines)),
            dma((3 * chips - 2, m)),
            dma((3, n)),
            dma((3, n)),
            dma((2, 2 * chips)),
            dma((2, n)),
            dma((chips,)),
            dma((chips,)),
            dma((chips, chips)),
            dma((chips, chips)),
            dma((chips,)),
            dma((chips,)),
            dma((chips, lines)),
            dma((chips, lines)),
            dma((chips, lines)),
            dma((chips, lines)),
            dma((chips, lines)),
            dma((5,)),
            dma((3, tiles)),
        ],
        cost_estimate=pl.CostEstimate(flops=flops, bytes_accessed=40 * slab * width, transcendentals=0),
        compiler_params=pltpu.CompilerParams(
            collective_id=cid, has_side_effects=True, vmem_limit_bytes=66_000_000
        ),
    )(activations, grad_out, gate_pre, up_pre, gate_w, up_w, down_w)


def per_device(activations, grad_out, gate_pre, up_pre, gate_up, down_weight):
    tokens, model = activations.shape
    gathered, grad_gate, grad_up, grad_down = layer(
        1, activations, grad_out, gate_pre, up_pre, gate_up[:, 0, :], gate_up[:, 1, :], down_weight
    )
    grad_input = gathered.transpose(1, 0, 2).reshape(tokens, model)
    grad_gate_up = jnp.stack([grad_gate, grad_up], axis=1).astype(F32)
    return (grad_input, grad_gate_up, grad_down.astype(F32))


def solution(mesh):
    in_specs = (
        P("dp", None),
        P("dp", None),
        P("dp", "tensor"),
        P("dp", "tensor"),
        P("dp", None, "tensor"),
        P("dp", "tensor"),
    )
    out_specs = (P("dp", None), P("dp", None, "tensor"), P("dp", "tensor"))
    return jax.shard_map(
        per_device, mesh=mesh, in_specs=in_specs, out_specs=out_specs, check_vma=False
    )
```

```python
import math

import jax
import jax.numpy as jnp
from jax import lax
from jax.experimental import pallas as pl
from jax.experimental.pallas import tpu as pltpu
from jax.sharding import PartitionSpec as P

MESH = pl.DeviceIdType.MESH
ANY = pl.BlockSpec(memory_space=pl.ANY)
F32 = jnp.float32
BF16 = jnp.bfloat16


def remote(src, dst, send, recv, device):
    return pltpu.make_async_remote_copy(
        src_ref=src, dst_ref=dst, send_sem=send, recv_sem=recv, device_id=device, device_id_type=MESH
    )


SCOPED = False


class Plain:
    def __enter__(self):
        return self

    def __exit__(self, *args):
        return None


def scope(name):
    return jax.named_scope(name) if SCOPED else Plain()


def tile_of(size):
    for tile in (256, 128):
        if size % tile == 0:
            return tile
    return size


class Line:
    def __init__(self, block, send, recv, j, m):
        self.block, self.send, self.recv = block, send, recv
        self.m, self.lines = m, m // 2
        self.row, self.column = j // 2, lax.rem(j, 2)
        self.facing = j + 1 - 2 * self.column
        self.above_me, self.below_me = lax.rem(j + 2, m), lax.rem(j + m - 2, m)
        self.first, self.last = self.row == 0, self.row == self.lines - 1

    def hop(self, kind, r, device):
        k = 2 * r + self.column
        block = self.block(k)
        return remote(block, block, self.send.at[kind, r], self.recv.at[k], {"tensor": device})

    def up(self, r):
        return self.hop(0, r, self.above_me)

    def down(self, r):
        return self.hop(1, r, self.below_me)

    def across(self, r):
        return self.hop(2, r, self.facing)

    def sideways(self):
        self.across(self.row).start()

    def lengthways(self):
        pl.when(jnp.logical_not(self.last))(lambda: self.up(self.row).start())
        pl.when(jnp.logical_not(self.first))(lambda: self.down(self.row).start())

    def step(self, d):
        if d == 0:
            self.lengthways()
            self.sideways()
            return
        below, above = self.row - d, self.row + d

        @pl.when(below >= 0)
        def _():
            self.up(below).wait_recv()
            pl.when(jnp.logical_not(self.last))(lambda: self.up(below).start())
            self.across(below).start()

        @pl.when(above < self.lines)
        def _():
            self.down(above).wait_recv()
            pl.when(jnp.logical_not(self.first))(lambda: self.down(above).start())
            self.across(above).start()

    def finish(self):
        for r in range(self.lines):
            k = 2 * r + 1 - self.column
            block = self.block(k)
            remote(
                block, block, self.send.at[2, r], self.recv.at[k], {"tensor": self.facing}
            ).wait_recv()

    def drain(self):
        for r in range(self.lines):
            self.across(r).wait_send()
            went_up = jnp.logical_and(jnp.logical_not(self.last), r <= self.row)
            went_down = jnp.logical_and(jnp.logical_not(self.first), r >= self.row)
            pl.when(went_up)(lambda: self.up(r).wait_send())
            pl.when(went_down)(lambda: self.down(r).wait_send())


def layer(cid, activations, grad_out, gate_pre, up_pre, gate_up, down_w):
    tokens, model = activations.shape
    slab, width = down_w.shape
    n = lax.axis_size("dp")
    m = lax.axis_size("tensor")
    chips, lines = n // 2, m // 2
    rows = tokens // m
    aligned = slab % 128 == 0
    if not aligned:
        activations, grad_out = (
            a.reshape(tokens, n, slab).transpose(1, 0, 2) for a in (activations, grad_out)
        )
    raw = width % 128 == 0
    mixed = (gate_up,) if raw else (gate_up[:, 0, :], gate_up[:, 1, :])
    tile = tile_of(slab)
    tiles = slab // tile
    lot = 16
    half = tokens // 2

    def kernel(*refs):
        single(refs[: len(mixed)], *refs[len(mixed) :])

    def single(
        mixed_in, x_in, dy_in, gate_in, up_in, down_in,
        out, wg0, wg1, wd,
        dy, x, gate, up, grad_h, down, both, w0, w1, gathered,
        keep, swap, pair, came, part, beside, carry, rising, falling, mine, final,
        wbuf,
        line_s, line_r, hop_s, hop_r, ge_s, ge_r, gx_s, gx_r, gf_s, gf_r, xs_s, xs_r,
        pair_s, pair_r, ex_s, ex_r, g_s, g_r,
        y_s, y_r, z_s, up_r, dn_r, load, store, leave,
    ):
        me = lax.axis_index("dp")
        j = lax.axis_index("tensor")
        core = lax.rem(me, 2)
        chip = me // 2
        partner = me + 1 - 2 * core
        z, y = j // 2, lax.rem(j, 2)
        facing = j + 1 - 2 * y
        above, below = lax.rem(j + 2, m), lax.rem(j + m - 2, m)
        first, last = z == 0, z == lines - 1
        others = list(range(1, chips))

        def shifted(s):
            return lax.rem(chip + s, chips)

        barrier = pltpu.get_barrier_semaphore()

        def signal(device):
            pl.semaphore_signal(barrier, inc=1, device_id=device, device_id_type=MESH)

        for s in range(1, n):
            signal({"dp": lax.rem(me + s, n)})
        signal({"tensor": facing})
        pl.when(jnp.logical_not(first))(lambda: signal({"tensor": below}))
        pl.when(jnp.logical_not(last))(lambda: signal({"tensor": above}))
        pl.semaphore_wait(barrier, n + (z > 0).astype(jnp.int32) + (z < lines - 1).astype(jnp.int32))

        my_half = pl.ds(pl.multiple_of(core * half, half), half)
        its_half = pl.ds(pl.multiple_of((1 - core) * half, half), half)
        my_rows = pl.ds(pl.multiple_of(j * rows, rows), rows)

        def cols_of(ref, r, p):
            if aligned:
                return ref.at[r, pl.ds(pl.multiple_of(p * slab, 128), slab)]
            return ref.at[p, r]

        def block(buf, p, k):
            return buf.at[p, pl.ds(pl.multiple_of(k * rows, rows), rows)]

        local_loads = [
            pltpu.make_async_copy(src, dst, load.at[i])
            for i, (src, dst) in enumerate(((down_in, down), (gate_in, gate.at[me]), (up_in, up.at[me])))
        ]
        weight_loads = [
            pltpu.make_async_copy(src, dst, load.at[3 + i])
            for i, (src, dst) in enumerate(
                ((mixed_in[0], both),) if raw else zip(mixed_in, (w0, w1))
            )
        ]

        def take_apart():
            for copy in weight_loads:
                copy.wait()
            if raw:

                @pl.loop(0, slab // lot)
                def _(i):
                    r = pl.ds(i * lot, lot)
                    flat = both[r].reshape(lot, 2 * width)
                    w0[r] = flat[:, :width]
                    w1[r] = flat[:, width:]

        def hop_copy(p):
            return remote(
                cols_of(dy_in, my_rows, p), block(dy, me, j), hop_s.at[0, p], hop_r.at[0, me], {"dp": p}
            )

        def near_copy(b, src, buf):
            return remote(
                cols_of(src, slice(None), partner),
                buf.at[me],
                hop_s.at[b, partner],
                hop_r.at[b, me],
                {"dp": partner},
            )

        def own_copy(b, src, buf):
            return pltpu.make_async_copy(cols_of(src, slice(None), me), buf.at[me], hop_s.at[b, me])

        def near_wait(b, src, buf):
            own_copy(b, src, buf).wait()
            spot = buf.at[partner]
            remote(spot, spot, hop_s.at[b, partner], hop_r.at[b, partner], {"dp": partner}).wait_recv()

        def x_copy(s, g, h):
            p = 2 * shifted(s) + g
            r = pl.ds(h * half, half)
            return remote(
                cols_of(x_in, r, p), x.at[me, r], xs_s.at[p, h], xs_r.at[me, h], {"dp": p}
            )

        def x_wait():
            near_wait(1, x_in, x)
            for s in others:
                for g in range(2):
                    for h in range(2):
                        q = 2 * shifted(s) + g
                        spot = x.at[q, pl.ds(h * half, half)]
                        remote(spot, spot, xs_s.at[q, h], xs_r.at[q, h], {"dp": q}).wait_recv()

        wide = ((gate_in, gate), (up_in, up))

        def wide_near(a):
            src, buf = wide[a]
            return remote(src, buf.at[me], ge_s.at[a], ge_r.at[a], {"dp": partner})

        def wide_near_wait(a):
            local_loads[1 + a].wait()
            spot = wide[a][1].at[partner]
            remote(spot, spot, ge_s.at[a], ge_r.at[a], {"dp": partner}).wait_recv()

        def wide_far(a, g, s):
            p = 2 * chip + g
            spot = wide[a][1].at[p, my_half]
            return remote(spot, spot, gx_s.at[a, g, s], gx_r.at[a, p], {"dp": 2 * shifted(s) + core})

        def wide_forward(a, p):
            spot = wide[a][1].at[p, my_half]
            return remote(spot, spot, gf_s.at[a, p], gf_r.at[a, p], {"dp": partner})

        def wide_far_wait(a, p):
            spot = wide[a][1].at[p, my_half]
            remote(spot, spot, gf_s.at[a, p], gx_r.at[a, p], {"dp": partner}).wait_recv()

        def wide_forward_wait(a, p):
            spot = wide[a][1].at[p, its_half]
            remote(spot, spot, gf_s.at[a, p], gf_r.at[a, p], {"dp": partner}).wait_recv()

        def lines_of(buf, base, shifts):
            made = []
            for g in range(2):
                for s in shifts:
                    i = base + len(made)
                    q = 2 * shifted(s) + g
                    made.append(
                        Line(lambda k, q=q: block(buf, q, k), line_s.at[i], line_r.at[i], j, m)
                    )
            return made

        dy_lines = lines_of(dy, 0, others)
        far_lines = lines_of(gathered, 2 * chips - 2, others)
        near_lines = lines_of(gathered, 4 * chips - 4, [0])

        def all_of(made, name, *args):
            for line in made:
                getattr(line, name)(*args)

        def pair_copy(p):
            return remote(swap.at[p], pair.at[p], pair_s.at[p], pair_r.at[p], {"dp": partner})

        def multiply(p):
            swap[p] = jnp.dot(dy[p, its_half], down[...], preferred_element_type=F32).astype(BF16)
            pair_copy(p).start()
            keep[p] = jnp.dot(dy[p, my_half], down[...], preferred_element_type=F32)

        def ex_copy(p, s):
            q = 2 * shifted(s) + core
            return remote(swap.at[p], came.at[chip, p], ex_s.at[p, s], ex_r.at[p, chip], {"dp": q})

        def chip_sum(p):
            pair_copy(p).wait()

            @pl.loop(0, half // lot)
            def _(i):
                r = pl.ds(i * lot, lot)
                total = keep[p, r] + pair[p, r].astype(F32)
                keep[p, r] = total
                swap[p, r] = total.astype(BF16)

            for s in others:
                ex_copy(p, s).start()

        def g_copy(p):
            spot = grad_h.at[p, my_half]
            return remote(spot, spot, g_s.at[p], g_r.at[p], {"dp": partner})

        def g_wait(p):
            spot = grad_h.at[p, its_half]
            remote(spot, spot, g_s.at[p], g_r.at[p], {"dp": partner}).wait_recv()

        def grad_h_sum(p):
            for s in others:
                q = shifted(s)
                spot = came.at[q, p]
                remote(spot, spot, ex_s.at[p, s], ex_r.at[p, q], {"dp": 2 * q + core}).wait_recv()

            @pl.loop(0, half // lot)
            def _(i):
                r = pl.ds(i * lot, lot)
                total = keep[p, r]
                for s in others:
                    total = total + came[shifted(s), p, r].astype(F32)
                grad_h[p, pl.ds(pl.multiple_of(core * half + i * lot, lot), lot)] = total.astype(BF16)

            g_copy(p).start()

        def gates(p):
            @pl.loop(0, tokens // lot)
            def _(i):
                r = pl.ds(i * lot, lot)
                v = gate[p, r].astype(F32)
                u = up[p, r].astype(F32)
                g = grad_h[p, r].astype(F32)
                s = jax.nn.sigmoid(v)
                silu = v * s
                grad_h[p, r] = (silu * u).astype(BF16)
                gate[p, r] = (g * u * s * (1.0 + v * (1.0 - s))).astype(BF16)
                up[p, r] = (g * silu).astype(BF16)

        def input_part(p):
            across = (((1,), (1,)), ((), ()))
            for i in range(tiles):
                cols = pl.ds(i * tile, tile)
                total = lax.dot_general(gate[p], w0[cols], across, preferred_element_type=F32)
                total = total + lax.dot_general(up[p], w1[cols], across, preferred_element_type=F32)
                part[p, :, cols] = total.astype(BF16)

        orders = [sorted(range(lines), key=lambda t: (-abs(t - r), t)) for r in range(lines)]

        def target(i):
            t = jnp.int32(0)
            for r in range(lines):
                t = jnp.where(z == r, orders[r][i], t)
            return t

        def y_copy(p, i):
            t = target(i)
            src = block(part, p, 2 * t + 1 - y)
            return remote(src, beside.at[p, t], y_s.at[p, t], y_r.at[p, t], {"tensor": facing})

        def climb(p, t):
            return remote(carry.at[p, t], rising.at[p, t], z_s.at[p, t], up_r.at[p, t], {"tensor": above})

        def descend(p, t):
            return remote(carry.at[p, t], falling.at[p, t], z_s.at[p, t], dn_r.at[p, t], {"tensor": below})

        def add_rows(fn):
            for i in range(rows // lot):
                fn(slice(i * lot, (i + 1) * lot), i * lot)

        def item(p, i):
            t = target(i)
            y_copy(p, i).wait_recv()
            rise = jnp.logical_and(t > z, z > 0)
            fall = jnp.logical_and(t < z, z < lines - 1)
            pl.when(rise)(lambda: climb(p, t).wait_recv())
            pl.when(fall)(lambda: descend(p, t).wait_recv())

            def start_of(r, r0):
                q = pl.ds(pl.multiple_of((2 * t + y) * rows + r0, lot), lot)
                return part[p, q].astype(F32) + beside[p, t, r].astype(F32)

            def plain(r, r0):
                carry[p, t, r] = start_of(r, r0).astype(BF16)

            def risen(r, r0):
                carry[p, t, r] = (start_of(r, r0) + rising[p, t, r].astype(F32)).astype(BF16)

            def fallen(r, r0):
                carry[p, t, r] = (start_of(r, r0) + falling[p, t, r].astype(F32)).astype(BF16)

            def own(r, r0):
                mine[p, r] = start_of(r, r0)

            pl.when(rise)(lambda: add_rows(risen))
            pl.when(fall)(lambda: add_rows(fallen))
            edge = jnp.logical_or(jnp.logical_and(first, t > z), jnp.logical_and(last, t < z))
            pl.when(edge)(lambda: add_rows(plain))
            pl.when(t == z)(lambda: add_rows(own))
            pl.when(t > z)(lambda: climb(p, t).start())
            pl.when(t < z)(lambda: descend(p, t).start())

        def total_of(p):
            pl.when(z > 0)(lambda: climb(p, z).wait_recv())
            pl.when(z < lines - 1)(lambda: descend(p, z).wait_recv())

            def close(parts):
                def fn(r, r0):
                    total = mine[p, r]
                    for ref in parts:
                        total = total + ref[p, z, r].astype(F32)
                    final[p, r] = total.astype(BF16)

                return fn

            pl.when(first)(lambda: add_rows(close((falling,))))
            pl.when(last)(lambda: add_rows(close((rising,))))
            inner = jnp.logical_not(jnp.logical_or(first, last))
            pl.when(inner)(lambda: add_rows(close((rising, falling))))

        def out_copy(p):
            return remote(final.at[p], block(gathered, me, j), hop_s.at[2, p], hop_r.at[2, me], {"dp": p})

        def out_local():
            return pltpu.make_async_copy(final.at[me], block(gathered, me, j), hop_s.at[2, me])

        def out_wait(q):
            spot = block(gathered, q, j)
            remote(spot, spot, hop_s.at[2, q], hop_r.at[2, q], {"dp": q}).wait_recv()

        grads = ((x, gate, wg0), (x, up, wg1), (dy, grad_h, wd))

        def stored(a, i):
            r = pl.ds(i * tile, tile)
            return pltpu.make_async_copy(wbuf.at[a, r], grads[a][2].at[r], store.at[a, i])

        def weights(a, i):
            over_rows = (((0,), (0,)), ((), ()))
            cols = pl.ds(i * tile, tile)
            left, right, _ = grads[a]
            total = lax.dot_general(
                left[:, :, cols].reshape(n * tokens, tile),
                right[...].reshape(n * tokens, width),
                over_rows,
                preferred_element_type=F32,
            )
            wbuf[a, cols] = (total * (1.0 / n)).astype(BF16)
            stored(a, i).start()

        local_loads[0].start()
        for s in others:
            for g in range(2):
                hop_copy(2 * shifted(s) + g).start()
        near_copy(0, dy_in, dy).start()
        own_copy(0, dy_in, dy).start()
        for a in range(2):
            wide_near(a).start()
            local_loads[1 + a].start()

        def send_wide(g):
            for a in range(2):
                for s in others:
                    wide_far(a, g, s).start()

        def afar(g):
            return [2 * shifted(s) + g for s in others]

        def chunk(p, far, tag):
            with scope("gsum" + tag):
                grad_h_sum(p)
            with scope("gwait" + tag):
                for a in range(2):
                    if far:
                        wide_forward(a, p).wait_send()
                        wide_forward_wait(a, p)
                    else:
                        for s in others:
                            wide_far(a, 1 if far is None else 0, s).wait_send()
                g_copy(p).wait_send()
                g_wait(p)
            with scope("gates" + tag):
                gates(p)
            with scope("part" + tag):
                input_part(p)
                for i in range(lines):
                    y_copy(p, i).start()

        def far_forward(g):
            with scope("fwd%d" % g):
                for p in afar(g):
                    for a in range(2):
                        wide_far_wait(a, p)
                        wide_forward(a, p).start()

        def far_chunk(g):
            for p in afar(g):
                chunk(p, True, "B%d" % g)

        def near_chunk(g):
            chunk(2 * chip + g, None if g else False, "A%d" % g)

        def items(ps, tag, which):
            for p in ps:
                for i in which:
                    with scope("item" + tag + str(i)):
                        item(p, i)

        def far_total(g):
            with scope("totalB%d" % g):
                for p in afar(g):
                    total_of(p)
                    out_copy(p).start()

        def near_total(g):
            with scope("totalA%d" % g):
                total_of(2 * chip + g)
                pl.when(core == g)(lambda: out_local().start())
                pl.when(core != g)(lambda: out_copy(partner).start())

        def send_x(g, h):
            for s in others:
                x_copy(s, g, h).start()

        spare = [(2, i) for i in range(tiles)]

        def some(count):
            for _ in range(count):
                if spare:
                    a, i = spare.pop(0)
                    with scope("w%d%d" % (a, i)):
                        weights(a, i)

        every = range(lines)
        with scope("wide"):
            wide_near_wait(0)
            wide_near_wait(1)
            send_wide(0)
        with scope("near"):
            near_wait(0, dy_in, dy)
            local_loads[0].wait()
        with scope("mul0"):
            multiply(2 * chip)
        with scope("dyhop"):
            for g in range(2):
                for q in afar(g):
                    spot = block(dy, q, j)
                    remote(spot, spot, hop_s.at[0, q], hop_r.at[0, q], {"dp": q}).wait_recv()
                all_of(dy_lines[g * (chips - 1) : (g + 1) * (chips - 1)], "step", 0)
        with scope("sum0"):
            chip_sum(2 * chip)
            send_wide(1)
            multiply(2 * chip + 1)
        if lines > 1:
            with scope("dy1"):
                all_of(dy_lines, "step", 1)
        with scope("sum0b"):
            chip_sum(2 * chip + 1)
        for copy in weight_loads:
            copy.start()
        near_copy(1, x_in, x).start()
        own_copy(1, x_in, x).start()
        for d in range(2, lines):
            with scope("dy%d" % d):
                all_of(dy_lines, "step", d)
            if d == 2:
                with scope("apart"):
                    take_apart()
        if lines <= 2:
            take_apart()
        for g in range(2):
            with scope("dyfin"):
                all_of(dy_lines[g * (chips - 1) : (g + 1) * (chips - 1)], "finish")
            with scope("mul1"):
                for p in afar(g):
                    multiply(p)
        with scope("sum1"):
            for g in range(2):
                for p in afar(g):
                    chip_sum(p)
        mid = lines // 2
        far_forward(0)
        far_chunk(0)
        items(afar(0), "B0", range(1))
        far_forward(1)
        far_chunk(1)
        items(afar(0), "B0", range(1, lines))
        near_chunk(0)
        send_x(0, 0)
        items(afar(1), "B1", range(1))
        near_chunk(1)
        far_total(0)
        items(afar(1), "B1", range(1, lines))
        items([2 * chip], "A0", range(mid))
        far_total(1)
        for g, h in ((0, 1), (1, 0), (1, 1)):
            send_x(g, h)
        items([2 * chip], "A0", range(mid, lines))
        some(1)
        items([2 * chip + 1], "A1", range(1))
        with scope("outB0"):
            for g in range(2):
                for q in afar(g):
                    out_wait(q)
            all_of(far_lines, "sideways")
        items([2 * chip + 1], "A1", range(1, lines))
        all_of(far_lines, "lengthways")
        near_total(0)
        some(1)
        near_total(1)
        if lines > 1:
            with scope("outB1"):
                all_of(far_lines, "step", 1)
        with scope("outA0"):
            out_wait(partner)
            out_local().wait()
            all_of(near_lines, "step", 0)
        for d in range(2, lines + 1):
            if d < lines:
                with scope("outB%d" % d):
                    all_of(far_lines, "step", d)
            some(2)
            if d == lines - 1:
                some(tiles)
                with scope("xwait"):
                    x_wait()
                spare += [(a, i) for i in range(tiles) for a in range(2)]
                some(1)
            with scope("outA%d" % (d - 1)):
                all_of(near_lines, "step", d - 1)
            some(2)
        some(2 * tiles)

        def leaving(q):
            return pltpu.make_async_copy(gathered.at[q], out.at[q], leave.at[q])

        for made, shifts in ((far_lines, others), (near_lines, [0])):
            with scope("outfin"):
                for i, line in enumerate(made):
                    line.finish()
                    leaving(2 * shifted(shifts[i % len(shifts)]) + i // len(shifts)).start()

        with scope("drain"):
            all_of(dy_lines + far_lines + near_lines, "drain")
            for g in range(2):
                for p in afar(g):
                    hop_copy(p).wait_send()
                    out_copy(p).wait_send()
                for s in others:
                    for h in range(2):
                        x_copy(s, g, h).wait_send()
            near_copy(0, dy_in, dy).wait_send()
            near_copy(1, x_in, x).wait_send()
            out_copy(partner).wait_send()
            for a in range(2):
                wide_near(a).wait_send()
            for s in range(chips):
                for g in range(2):
                    p = 2 * shifted(s) + g
                    for u in others:
                        ex_copy(p, u).wait_send()
                    for i in every:
                        y_copy(p, i).wait_send()
                        t = target(i)
                        pl.when(t > z)(lambda: climb(p, t).wait_send())
                        pl.when(t < z)(lambda: descend(p, t).wait_send())
        with scope("stores"):
            for q in range(n):
                leaving(q).wait()
            for a in range(3):
                for i in range(tiles):
                    stored(a, i).wait()

    dma = pltpu.SemaphoreType.DMA
    vm = pltpu.VMEM
    flops = 2 * n * tokens * slab * width * 6
    return pl.pallas_call(
        kernel,
        out_shape=[jax.ShapeDtypeStruct((n, tokens, slab), BF16)]
        + [jax.ShapeDtypeStruct((slab, width), BF16)] * 3,
        in_specs=[ANY] * (5 + len(mixed)),
        out_specs=[ANY] * 4,
        scratch_shapes=[
            vm((n, tokens, slab), BF16),
            vm((n, tokens, slab), BF16),
            vm((n, tokens, width), BF16),
            vm((n, tokens, width), BF16),
            vm((n, tokens, width), BF16),
            vm((slab, width), BF16),
            vm((slab, 2, width) if raw else (16, 128), BF16),
            vm((slab, width), BF16),
            vm((slab, width), BF16),
            vm((n, tokens, slab), BF16),
            vm((n, half, width), F32),
            vm((n, half, width), BF16),
            vm((n, half, width), BF16),
            vm((chips, n, half, width), BF16),
            vm((n, tokens, slab), BF16),
            vm((n, lines, rows, slab), BF16),
            vm((n, lines, rows, slab), BF16),
            vm((n, lines, rows, slab), BF16),
            vm((n, lines, rows, slab), BF16),
            vm((n, rows, slab), F32),
            vm((n, rows, slab), BF16),
            vm((3, slab, width), BF16),
            dma((4 * chips - 2, 3, lines)),
            dma((4 * chips - 2, m)),
            dma((3, n)),
            dma((3, n)),
            dma((2,)),
            dma((2,)),
            dma((2, 2, chips)),
            dma((2, n)),
            dma((2, n)),
            dma((2, n)),
            dma((n, 2)),
            dma((n, 2)),
            dma((n,)),
            dma((n,)),
            dma((n, chips)),
            dma((n, chips)),
            dma((n,)),
            dma((n,)),
            dma((n, lines)),
            dma((n, lines)),
            dma((n, lines)),
            dma((n, lines)),
            dma((n, lines)),
            dma((5,)),
            dma((3, tiles)),
            dma((n,)),
        ],
        cost_estimate=pl.CostEstimate(flops=flops, bytes_accessed=40 * slab * width, transcendentals=0),
        compiler_params=pltpu.CompilerParams(
            collective_id=cid, has_side_effects=True, vmem_limit_bytes=66_000_000
        ),
    )(*mixed, activations, grad_out, gate_pre, up_pre, down_w)


def spread_out(gathered, grad_gate, grad_up, grad_down):
    n, tokens, slab = gathered.shape
    width = grad_down.shape[1]
    steps = min(math.gcd(tokens // 16, slab // 16), 4)
    t, r = tokens // steps, slab // steps

    def kernel(all_ref, gate_ref, up_ref, down_ref, input_ref, pair_ref, last_ref):
        for q in range(n):
            input_ref[:, q * slab : (q + 1) * slab] = all_ref[q]
        pair_ref[:, 0, :] = gate_ref[...].astype(F32)
        pair_ref[:, 1, :] = up_ref[...].astype(F32)
        last_ref[...] = down_ref[...].astype(F32)

    flat = pl.BlockSpec((r, width), lambda i: (i, 0))
    return pl.pallas_call(
        kernel,
        grid=(steps,),
        out_shape=[
            jax.ShapeDtypeStruct((tokens, n * slab), BF16),
            jax.ShapeDtypeStruct((slab, 2, width), F32),
            jax.ShapeDtypeStruct((slab, width), F32),
        ],
        in_specs=[pl.BlockSpec((n, t, slab), lambda i: (0, i, 0)), flat, flat, flat],
        out_specs=[
            pl.BlockSpec((t, n * slab), lambda i: (i, 0)),
            pl.BlockSpec((r, 2, width), lambda i: (i, 0, 0)),
            flat,
        ],
        cost_estimate=pl.CostEstimate(
            flops=slab * width, bytes_accessed=18 * slab * width, transcendentals=0
        ),
    )(gathered, grad_gate, grad_up, grad_down)


def per_device(activations, grad_out, gate_pre, up_pre, gate_up, down_weight):
    made = layer(1, activations, grad_out, gate_pre, up_pre, gate_up, down_weight)
    return tuple(spread_out(*made))


def solution(mesh):
    in_specs = (
        P("dp", None),
        P("dp", None),
        P("dp", "tensor"),
        P("dp", "tensor"),
        P("dp", None, "tensor"),
        P("dp", "tensor"),
    )
    out_specs = (P("dp", None), P("dp", None, "tensor"), P("dp", "tensor"))
    return jax.shard_map(
        per_device, mesh=mesh, in_specs=in_specs, out_specs=out_specs, check_vma=False
    )
```

```python
import math

import jax
import jax.numpy as jnp
from jax import lax
from jax.experimental import pallas as pl
from jax.experimental.pallas import tpu as pltpu
from jax.sharding import PartitionSpec as P

MESH = pl.DeviceIdType.MESH
ANY = pl.BlockSpec(memory_space=pl.ANY)
F32 = jnp.float32
BF16 = jnp.bfloat16


def remote(src, dst, send, recv, device):
    return pltpu.make_async_remote_copy(
        src_ref=src, dst_ref=dst, send_sem=send, recv_sem=recv, device_id=device, device_id_type=MESH
    )


SCOPED = False


class Plain:
    def __enter__(self):
        return self

    def __exit__(self, *args):
        return None


def scope(name):
    return jax.named_scope(name) if SCOPED else Plain()


def tile_of(size):
    for tile in (256, 128):
        if size % tile == 0:
            return tile
    return size


def pick(z, values):
    chosen = jnp.int32(0)
    for r, value in enumerate(values):
        chosen = jnp.where(z == r, value, chosen)
    return chosen


class Line:
    def __init__(self, block, bulk, send, recv, j, m):
        self.block, self.bulk, self.send, self.recv = block, bulk, send, recv
        self.m, self.lines = m, m // 2
        self.row, self.column = j // 2, lax.rem(j, 2)
        self.facing = j + 1 - 2 * self.column
        self.above_me, self.below_me = lax.rem(j + 2, m), lax.rem(j + m - 2, m)
        self.first, self.last = self.row == 0, self.row == self.lines - 1

    def hop(self, send, recv, r, device):
        block = self.block(2 * r + self.column)
        return remote(block, block, self.send.at[send], self.recv.at[recv], {"tensor": device})

    def up(self, r):
        return self.hop(r, r, r, self.above_me)

    def down(self, r):
        return self.hop(jnp.where(r == self.row, self.lines, r), r, r, self.below_me)

    def across(self, r):
        return self.hop(self.lines + 1, self.lines, r, self.facing)

    def all_across(self):
        send, recv = self.send.at[self.lines + 1], self.recv.at[self.lines]
        return remote(self.bulk, self.bulk, send, recv, {"tensor": self.facing})

    def sideways(self):
        self.across(self.row).start()

    def lengthways(self):
        pl.when(jnp.logical_not(self.last))(lambda: self.up(self.row).start())
        pl.when(jnp.logical_not(self.first))(lambda: self.down(self.row).start())

    def step(self, d):
        if d == 0:
            self.lengthways()
            self.sideways()
            return
        below, above = self.row - d, self.row + d

        @pl.when(below >= 0)
        def _():
            self.up(below).wait_recv()
            pl.when(jnp.logical_not(self.last))(lambda: self.up(below).start())
            self.across(below).start()

        @pl.when(above < self.lines)
        def _():
            self.down(above).wait_recv()
            pl.when(jnp.logical_not(self.first))(lambda: self.down(above).start())
            self.across(above).start()

    def finish(self):
        self.all_across().wait_recv()

    def drain(self):
        self.all_across().wait_send()
        for r in range(self.lines):
            went_up = jnp.logical_and(jnp.logical_not(self.last), r <= self.row)
            went_down = jnp.logical_and(jnp.logical_not(self.first), r >= self.row)
            pl.when(went_up)(lambda: self.up(r).wait_send())
            pl.when(went_down)(lambda: self.down(r).wait_send())


def layer(cid, activations, grad_out, gate_pre, up_pre, gate_up, down_w):
    tokens, model = activations.shape
    slab, width = down_w.shape
    n = lax.axis_size("dp")
    m = lax.axis_size("tensor")
    chips, lines = n // 2, m // 2
    rows = tokens // m
    aligned = slab % 128 == 0
    if not aligned:
        activations, grad_out = (
            a.reshape(tokens, n, slab).transpose(1, 0, 2) for a in (activations, grad_out)
        )
    raw = width % 128 == 0
    mixed = (gate_up,) if raw else (gate_up[:, 0, :], gate_up[:, 1, :])
    tile = tile_of(slab)
    tiles = slab // tile
    lot = 16
    half = tokens // 2

    def kernel(*refs):
        single(refs[: len(mixed)], *refs[len(mixed) :])

    def single(
        mixed_in, x_in, dy_in, gate_in, up_in, down_in,
        out, wg0, wg1, wd,
        dy, x, gate, up, grad_h, down, both, w0, w1, gathered,
        keep, swap, pair, came, part, beside, carry, rising, mine, final,
        wbuf,
        line_s, line_r, hop_s, hop_r, ge_s, ge_r, gx_s, gx_r, gf_s, gf_r, xs_s, xs_r,
        pair_s, pair_r, ex_s, ex_r, g_s, g_r,
        y_s, y_r, z_s, z_r, load, store, leave,
    ):
        me = lax.axis_index("dp")
        j = lax.axis_index("tensor")
        core = lax.rem(me, 2)
        chip = me // 2
        partner = me + 1 - 2 * core
        z, y = j // 2, lax.rem(j, 2)
        facing = j + 1 - 2 * y
        others = list(range(1, chips))

        def shifted(s):
            return lax.rem(chip + s, chips)

        barrier = pltpu.get_barrier_semaphore()

        def signal(device):
            pl.semaphore_signal(barrier, inc=1, device_id=device, device_id_type=MESH)

        for s in range(1, n):
            signal({"dp": lax.rem(me + s, n)})
        signal({"tensor": facing})
        for d in range(1, lines):
            signal({"tensor": lax.rem(j + 2 * d, m)})
        pl.semaphore_wait(barrier, n + lines - 1)

        my_half = pl.ds(pl.multiple_of(core * half, half), half)
        its_half = pl.ds(pl.multiple_of((1 - core) * half, half), half)
        my_rows = pl.ds(pl.multiple_of(j * rows, rows), rows)

        def cols_of(ref, r, p):
            if aligned:
                return ref.at[r, pl.ds(pl.multiple_of(p * slab, 128), slab)]
            return ref.at[p, r]

        def block(buf, p, k):
            return buf.at[p, pl.ds(pl.multiple_of(k * rows, rows), rows)]

        local_loads = [
            pltpu.make_async_copy(src, dst, load.at[i])
            for i, (src, dst) in enumerate(((down_in, down), (gate_in, gate.at[me]), (up_in, up.at[me])))
        ]
        weight_loads = [
            pltpu.make_async_copy(src, dst, load.at[3 + i])
            for i, (src, dst) in enumerate(
                ((mixed_in[0], both),) if raw else zip(mixed_in, (w0, w1))
            )
        ]

        def take_apart():
            for copy in weight_loads:
                copy.wait()
            if raw:

                @pl.loop(0, slab // lot)
                def _(i):
                    r = pl.ds(i * lot, lot)
                    flat = both[r].reshape(lot, 2 * width)
                    w0[r] = flat[:, :width]
                    w1[r] = flat[:, width:]

        def hop_copy(p):
            return remote(
                cols_of(dy_in, my_rows, p), block(dy, me, j), hop_s.at[0, p], hop_r.at[0, me], {"dp": p}
            )

        def near_copy(b, src, buf):
            return remote(
                cols_of(src, slice(None), partner),
                buf.at[me],
                hop_s.at[b, partner],
                hop_r.at[b, me],
                {"dp": partner},
            )

        def own_copy(b, src, buf):
            return pltpu.make_async_copy(cols_of(src, slice(None), me), buf.at[me], hop_s.at[b, me])

        def near_wait(b, src, buf):
            own_copy(b, src, buf).wait()
            spot = buf.at[partner]
            remote(spot, spot, hop_s.at[b, partner], hop_r.at[b, partner], {"dp": partner}).wait_recv()

        def x_copy(s, g, h):
            p = 2 * shifted(s) + g
            r = pl.ds(h * half, half)
            return remote(
                cols_of(x_in, r, p), x.at[me, r], xs_s, xs_r.at[me], {"dp": p}
            )

        def x_wait():
            near_wait(1, x_in, x)
            for s in others:
                for g in range(2):
                    q = 2 * shifted(s) + g
                    remote(x.at[q], x.at[q], xs_s, xs_r.at[q], {"dp": q}).wait_recv()

        wide = ((gate_in, gate), (up_in, up))

        def wide_near(a):
            src, buf = wide[a]
            return remote(src, buf.at[me], ge_s.at[a], ge_r.at[a], {"dp": partner})

        def wide_near_wait(a):
            local_loads[1 + a].wait()
            spot = wide[a][1].at[partner]
            remote(spot, spot, ge_s.at[a], ge_r.at[a], {"dp": partner}).wait_recv()

        def wide_far(a, g, s):
            p = 2 * chip + g
            spot = wide[a][1].at[p, my_half]
            return remote(spot, spot, gx_s.at[a, g, s - 1], gx_r.at[a, p], {"dp": 2 * shifted(s) + core})

        def wide_forward(a, p):
            spot = wide[a][1].at[p, my_half]
            return remote(spot, spot, gf_s.at[a, p], gf_r.at[a, p], {"dp": partner})

        def wide_far_wait(a, p):
            spot = wide[a][1].at[p, my_half]
            remote(spot, spot, gf_s.at[a, p], gx_r.at[a, p], {"dp": partner}).wait_recv()

        def wide_forward_wait(a, p):
            spot = wide[a][1].at[p, its_half]
            remote(spot, spot, gf_s.at[a, p], gf_r.at[a, p], {"dp": partner}).wait_recv()

        def lines_of(buf, base, shifts):
            made = []
            for g in range(2):
                for s in shifts:
                    i = base + len(made)
                    q = 2 * shifted(s) + g
                    made.append(
                        Line(
                            lambda k, q=q: block(buf, q, k),
                            buf.at[q, pl.ds(0, half)],
                            line_s.at[i],
                            line_r.at[i],
                            j,
                            m,
                        )
                    )
            return made

        dy_lines = lines_of(dy, 0, others)
        far_lines = lines_of(gathered, 2 * chips - 2, others)
        near_lines = lines_of(gathered, 4 * chips - 4, [0])

        def all_of(made, name, *args):
            for line in made:
                getattr(line, name)(*args)

        def pair_copy(p):
            return remote(swap.at[p], pair.at[p], pair_s.at[p], pair_r.at[p], {"dp": partner})

        def multiply(p):
            swap[p] = jnp.dot(dy[p, its_half], down[...], preferred_element_type=F32).astype(BF16)
            pair_copy(p).start()
            keep[p] = jnp.dot(dy[p, my_half], down[...], preferred_element_type=F32)

        def ex_copy(p, s):
            q = 2 * shifted(s) + core
            return remote(swap.at[p], came.at[chip, p], ex_s.at[p, s - 1], ex_r.at[p, s - 1], {"dp": q})

        def chip_sum(p):
            pair_copy(p).wait()

            @pl.loop(0, half // lot)
            def _(i):
                r = pl.ds(i * lot, lot)
                total = keep[p, r] + pair[p, r].astype(F32)
                keep[p, r] = total
                swap[p, r] = total.astype(BF16)

            for s in others:
                ex_copy(p, s).start()

        def g_copy(p):
            spot = grad_h.at[p, my_half]
            return remote(spot, spot, g_s.at[p], g_r.at[p], {"dp": partner})

        def g_wait(p):
            spot = grad_h.at[p, its_half]
            remote(spot, spot, g_s.at[p], g_r.at[p], {"dp": partner}).wait_recv()

        def grad_h_sum(p):
            for s in others:
                q = shifted(s)
                spot = came.at[q, p]
                u = chips - s - 1
                remote(spot, spot, ex_s.at[p, u], ex_r.at[p, u], {"dp": 2 * q + core}).wait_recv()

            @pl.loop(0, half // lot)
            def _(i):
                r = pl.ds(i * lot, lot)
                total = keep[p, r]
                for s in others:
                    total = total + came[shifted(s), p, r].astype(F32)
                grad_h[p, pl.ds(pl.multiple_of(core * half + i * lot, lot), lot)] = total.astype(BF16)

            g_copy(p).start()

        def gates(p):
            @pl.loop(0, tokens // lot)
            def _(i):
                r = pl.ds(i * lot, lot)
                v = gate[p, r].astype(F32)
                u = up[p, r].astype(F32)
                g = grad_h[p, r].astype(F32)
                s = jax.nn.sigmoid(v)
                silu = v * s
                grad_h[p, r] = (silu * u).astype(BF16)
                gate[p, r] = (g * u * s * (1.0 + v * (1.0 - s))).astype(BF16)
                up[p, r] = (g * silu).astype(BF16)

        def input_part(p):
            across = (((1,), (1,)), ((), ()))
            for i in range(tiles):
                cols = pl.ds(i * tile, tile)
                total = lax.dot_general(gate[p], w0[cols], across, preferred_element_type=F32)
                total = total + lax.dot_general(up[p], w1[cols], across, preferred_element_type=F32)
                part[p, :, cols] = total.astype(BF16)

        orders = [sorted(range(lines), key=lambda t: (-abs(t - r), t)) for r in range(lines)]

        def target(i):
            return pick(z, [order[i] for order in orders])

        def y_copy(p, i):
            t = target(i)
            src = block(part, p, 2 * t + 1 - y)
            return remote(src, beside.at[p, t], y_s.at[p], y_r.at[p, t], {"tensor": facing})

        def z_copy(p, t):
            return remote(
                carry.at[p, t], rising.at[p, z], z_s.at[p], z_r.at[p], {"tensor": 2 * t + y}
            )

        def z_all(p):
            spot = carry.at[p, pl.ds(0, lines - 1)]
            return remote(spot, spot, z_s.at[p], z_r.at[p], {"tensor": facing})

        def item(p, i):
            t = target(i)
            y_copy(p, i).wait_recv()
            for i0 in range(0, rows, lot):
                r = slice(i0, i0 + lot)
                q = pl.ds(pl.multiple_of((2 * t + y) * rows + i0, lot), lot)
                total = part[p, q].astype(F32) + beside[p, t, r].astype(F32)
                if i < lines - 1:
                    carry[p, t, r] = total.astype(BF16)
                else:
                    mine[p, r] = total
            if i < lines - 1:
                z_copy(p, t).start()

        def total_of(p):
            sources = [lax.rem(z + d, lines) for d in range(1, lines)]
            if lines > 1:
                z_all(p).wait_recv()
            for i0 in range(0, rows, lot):
                r = slice(i0, i0 + lot)
                total = mine[p, r]
                for q in sources:
                    total = total + rising[p, q, r].astype(F32)
                final[p, r] = total.astype(BF16)

        def out_copy(p):
            return remote(final.at[p], block(gathered, me, j), hop_s.at[2, p], hop_r.at[2, me], {"dp": p})

        def out_local():
            return pltpu.make_async_copy(final.at[me], block(gathered, me, j), hop_s.at[2, me])

        def out_wait(q):
            spot = block(gathered, q, j)
            remote(spot, spot, hop_s.at[2, q], hop_r.at[2, q], {"dp": q}).wait_recv()

        grads = ((x, gate, wg0), (x, up, wg1), (dy, grad_h, wd))

        def stored(a, i):
            r = pl.ds(i * tile, tile)
            return pltpu.make_async_copy(wbuf.at[a, r], grads[a][2].at[r], store.at[a])

        def weights(a, i):
            over_rows = (((0,), (0,)), ((), ()))
            cols = pl.ds(i * tile, tile)
            left, right, _ = grads[a]
            total = lax.dot_general(
                left[:, :, cols].reshape(n * tokens, tile),
                right[...].reshape(n * tokens, width),
                over_rows,
                preferred_element_type=F32,
            )
            wbuf[a, cols] = (total * (1.0 / n)).astype(BF16)
            stored(a, i).start()

        local_loads[0].start()
        for s in others:
            for g in range(2):
                hop_copy(2 * shifted(s) + g).start()
        near_copy(0, dy_in, dy).start()
        own_copy(0, dy_in, dy).start()
        for a in range(2):
            wide_near(a).start()
            local_loads[1 + a].start()

        def send_wide(g):
            for a in range(2):
                for s in others:
                    wide_far(a, g, s).start()

        def afar(g):
            return [2 * shifted(s) + g for s in others]

        def chunk(p, far, tag):
            with scope("gsum" + tag):
                grad_h_sum(p)
            with scope("gwait" + tag):
                for a in range(2):
                    if far:
                        wide_forward(a, p).wait_send()
                        wide_forward_wait(a, p)
                    else:
                        for s in others:
                            wide_far(a, 1 if far is None else 0, s).wait_send()
                g_copy(p).wait_send()
                g_wait(p)
            with scope("gates" + tag):
                gates(p)
            with scope("part" + tag):
                input_part(p)
                for i in range(lines):
                    y_copy(p, i).start()

        def far_forward(g):
            with scope("fwd%d" % g):
                for p in afar(g):
                    for a in range(2):
                        wide_far_wait(a, p)
                        wide_forward(a, p).start()

        def far_chunk(g):
            for p in afar(g):
                chunk(p, True, "B%d" % g)

        def near_chunk(g):
            chunk(2 * chip + g, None if g else False, "A%d" % g)

        def items(ps, tag, which):
            for p in ps:
                for i in which:
                    with scope("item" + tag + str(i)):
                        item(p, i)

        def far_total(g):
            with scope("totalB%d" % g):
                for p in afar(g):
                    total_of(p)
                    out_copy(p).start()

        def near_total(g):
            with scope("totalA%d" % g):
                total_of(2 * chip + g)
                pl.when(core == g)(lambda: out_local().start())
                pl.when(core != g)(lambda: out_copy(partner).start())

        def send_x(g, h):
            for s in others:
                x_copy(s, g, h).start()

        spare = [(2, i) for i in range(tiles)]

        def some(count):
            for _ in range(count):
                if spare:
                    a, i = spare.pop(0)
                    with scope("w%d%d" % (a, i)):
                        weights(a, i)

        every = range(lines)
        with scope("wide"):
            wide_near_wait(0)
            wide_near_wait(1)
            send_wide(0)
        with scope("near"):
            near_wait(0, dy_in, dy)
            local_loads[0].wait()
        with scope("mul0"):
            multiply(2 * chip)
        with scope("dyhop"):
            for g in range(2):
                for q in afar(g):
                    spot = block(dy, q, j)
                    remote(spot, spot, hop_s.at[0, q], hop_r.at[0, q], {"dp": q}).wait_recv()
                all_of(dy_lines[g * (chips - 1) : (g + 1) * (chips - 1)], "step", 0)
        with scope("sum0"):
            chip_sum(2 * chip)
            send_wide(1)
            multiply(2 * chip + 1)
        if lines > 1:
            with scope("dy1"):
                all_of(dy_lines, "step", 1)
        with scope("sum0b"):
            chip_sum(2 * chip + 1)
        for copy in weight_loads:
            copy.start()
        near_copy(1, x_in, x).start()
        own_copy(1, x_in, x).start()
        for d in range(2, lines):
            with scope("dy%d" % d):
                all_of(dy_lines, "step", d)
            if d == 2:
                with scope("apart"):
                    take_apart()
        if lines <= 2:
            take_apart()
        for g in range(2):
            with scope("dyfin"):
                all_of(dy_lines[g * (chips - 1) : (g + 1) * (chips - 1)], "finish")
            with scope("mul1"):
                for p in afar(g):
                    multiply(p)
        with scope("sum1"):
            for g in range(2):
                for p in afar(g):
                    chip_sum(p)
        mid = lines // 2
        far_forward(0)
        far_chunk(0)
        items(afar(0), "B0", range(1))
        far_forward(1)
        far_chunk(1)
        items(afar(0), "B0", range(1, lines))
        near_chunk(0)
        send_x(0, 0)
        items(afar(1), "B1", range(1))
        near_chunk(1)
        far_total(0)
        send_x(0, 1)
        items(afar(1), "B1", range(1, lines))
        items([2 * chip], "A0", range(mid))
        far_total(1)
        send_x(1, 0)
        send_x(1, 1)
        items([2 * chip], "A0", range(mid, lines))
        some(1)

        def open_near():
            out_wait(partner)
            out_local().wait()
            all_of(near_lines, "step", 0)

        def far_arrived():
            for g in range(2):
                for q in afar(g):
                    out_wait(q)
            all_of(far_lines, "sideways")

        with scope("farE"):
            pl.when(core == 0)(far_arrived)
        items([2 * chip + 1], "A1", every)
        with scope("farL"):
            pl.when(core == 1)(far_arrived)
            all_of(far_lines, "lengthways")
        near_total(0)
        with scope("nearE"):
            pl.when(core == 0)(open_near)
        some(1)
        near_total(1)
        with scope("nearL"):
            pl.when(core == 1)(open_near)
        if lines > 1:
            with scope("outB1"):
                all_of(far_lines, "step", 1)
        for d in range(2, lines + 1):
            if d < lines:
                with scope("outB%d" % d):
                    all_of(far_lines, "step", d)
            some(2)
            if d == lines - 1:
                some(tiles)
                with scope("xwait"):
                    x_wait()
                spare += [(a, i) for i in range(tiles) for a in range(2)]
                some(1)
            with scope("outA%d" % (d - 1)):
                all_of(near_lines, "step", d - 1)
            some(2)
        some(2 * tiles)

        def leaving(q):
            return pltpu.make_async_copy(gathered.at[q], out.at[q], leave.at[q])

        for made, shifts in ((far_lines, others), (near_lines, [0])):
            with scope("outfin"):
                for i, line in enumerate(made):
                    line.finish()
                    leaving(2 * shifted(shifts[i % len(shifts)]) + i // len(shifts)).start()

        with scope("drain"):
            all_of(dy_lines + far_lines + near_lines, "drain")
            for g in range(2):
                for p in afar(g):
                    hop_copy(p).wait_send()
                    out_copy(p).wait_send()
            if others:
                spot = x.at[pl.ds(0, n - 2)]
                remote(spot, spot, xs_s, xs_r.at[me], {"dp": partner}).wait_send()
            near_copy(0, dy_in, dy).wait_send()
            near_copy(1, x_in, x).wait_send()
            out_copy(partner).wait_send()
            for a in range(2):
                wide_near(a).wait_send()
            for s in range(chips):
                for g in range(2):
                    p = 2 * shifted(s) + g
                    for u in others:
                        ex_copy(p, u).wait_send()
                    spot = part.at[p, pl.ds(0, half)]
                    remote(spot, spot, y_s.at[p], y_r.at[p, 0], {"tensor": facing}).wait_send()
                    if lines > 1:
                        z_all(p).wait_send()
        with scope("stores"):
            for q in range(n):
                leaving(q).wait()
            for a in range(3):
                pltpu.make_async_copy(wbuf.at[a], grads[a][2], store.at[a]).wait()

    dma = pltpu.SemaphoreType.DMA
    vm = pltpu.VMEM
    flops = 2 * n * tokens * slab * width * 6
    return pl.pallas_call(
        kernel,
        out_shape=[jax.ShapeDtypeStruct((n, tokens, slab), BF16)]
        + [jax.ShapeDtypeStruct((slab, width), BF16)] * 3,
        in_specs=[ANY] * (5 + len(mixed)),
        out_specs=[ANY] * 4,
        scratch_shapes=[
            vm((n, tokens, slab), BF16),
            vm((n, tokens, slab), BF16),
            vm((n, tokens, width), BF16),
            vm((n, tokens, width), BF16),
            vm((n, tokens, width), BF16),
            vm((slab, width), BF16),
            vm((slab, 2, width) if raw else (16, 128), BF16),
            vm((slab, width), BF16),
            vm((slab, width), BF16),
            vm((n, tokens, slab), BF16),
            vm((n, half, width), F32),
            vm((n, half, width), BF16),
            vm((n, half, width), BF16),
            vm((chips, n, half, width), BF16),
            vm((n, tokens, slab), BF16),
            vm((n, lines, rows, slab), BF16),
            vm((n, lines, rows, slab), BF16),
            vm((n, lines, rows, slab), BF16),
            vm((n, rows, slab), F32),
            vm((n, rows, slab), BF16),
            vm((3, slab, width), BF16),
            dma((4 * chips - 2, lines + 2)),
            dma((4 * chips - 2, lines + 1)),
            dma((3, n)),
            dma((3, n)),
            dma((2,)),
            dma((2,)),
            dma((2, 2, max(chips - 1, 1))),
            dma((2, n)),
            dma((2, n)),
            dma((2, n)),
            dma,
            dma((n,)),
            dma((n,)),
            dma((n,)),
            dma((n, max(chips - 1, 1))),
            dma((n, max(chips - 1, 1))),
            dma((n,)),
            dma((n,)),
            dma((n,)),
            dma((n, lines)),
            dma((n,)),
            dma((n,)),
            dma((5,)),
            dma((3,)),
            dma((n,)),
        ],
        cost_estimate=pl.CostEstimate(flops=flops, bytes_accessed=40 * slab * width, transcendentals=0),
        compiler_params=pltpu.CompilerParams(
            collective_id=cid, has_side_effects=True, vmem_limit_bytes=66_000_000
        ),
    )(*mixed, activations, grad_out, gate_pre, up_pre, down_w)


def spread_out(gathered, grad_gate, grad_up, grad_down):
    n, tokens, slab = gathered.shape
    width = grad_down.shape[1]
    steps = min(math.gcd(tokens // 16, slab // 16), 4)
    t, r = tokens // steps, slab // steps

    def kernel(all_ref, gate_ref, up_ref, down_ref, input_ref, pair_ref, last_ref):
        for q in range(n):
            input_ref[:, q * slab : (q + 1) * slab] = all_ref[q]
        pair_ref[:, 0, :] = gate_ref[...].astype(F32)
        pair_ref[:, 1, :] = up_ref[...].astype(F32)
        last_ref[...] = down_ref[...].astype(F32)

    flat = pl.BlockSpec((r, width), lambda i: (i, 0))
    return pl.pallas_call(
        kernel,
        grid=(steps,),
        out_shape=[
            jax.ShapeDtypeStruct((tokens, n * slab), BF16),
            jax.ShapeDtypeStruct((slab, 2, width), F32),
            jax.ShapeDtypeStruct((slab, width), F32),
        ],
        in_specs=[pl.BlockSpec((n, t, slab), lambda i: (0, i, 0)), flat, flat, flat],
        out_specs=[
            pl.BlockSpec((t, n * slab), lambda i: (i, 0)),
            pl.BlockSpec((r, 2, width), lambda i: (i, 0, 0)),
            flat,
        ],
        cost_estimate=pl.CostEstimate(
            flops=slab * width, bytes_accessed=18 * slab * width, transcendentals=0
        ),
    )(gathered, grad_gate, grad_up, grad_down)


def per_device(activations, grad_out, gate_pre, up_pre, gate_up, down_weight):
    made = layer(1, activations, grad_out, gate_pre, up_pre, gate_up, down_weight)
    return tuple(spread_out(*made))


def solution(mesh):
    in_specs = (
        P("dp", None),
        P("dp", None),
        P("dp", "tensor"),
        P("dp", "tensor"),
        P("dp", None, "tensor"),
        P("dp", "tensor"),
    )
    out_specs = (P("dp", None), P("dp", None, "tensor"), P("dp", "tensor"))
    return jax.shard_map(
        per_device, mesh=mesh, in_specs=in_specs, out_specs=out_specs, check_vma=False
    )
```
